32 devices in a mesh: segment: 4 (over z), row: 4 (over y, x), col: 2 (over core).
Axes of the slice: x: 2, y: 2, z: 4, core: 2. Of those that a mesh axis runs over, the one named last changes fastest.
Arguments:
- frames: bfloat16 [2, 64, 32, 128], P(None, 'row', 'col'), may hold values from -6 to 6
- caches: bfloat16 [4, 2, 2, 64, 32, 128], P('segment', None, None, 'row', 'col'), may hold values from -5 to 5
- weights: bfloat16 [4, 2, 3, 3, 3, 128, 128], P('segment'), may hold values from -0.109375 to 0.109375
- biases: float32 [4, 2, 128], P('segment'), may hold values from -0.5 to 0.5
- gains: float32 [4, 2, 128], P('segment'), may hold values from 0.1 to 1.9
Outputs:
- sections: bfloat16 [4, 2, 64, 32, 128], P('segment', None, 'row', 'col')
The draws below stay inside these ranges and needn't reach their ends.
All inputs are finite; a program needn't handle non-finite values.
Results may differ from the reference program's by a relative error of at most 0.0055.
Values may be sent and summed in bfloat16 or wider, within the bound.
A program may use at most 64 MiB of HBM per device.

```python
import jax
import jax.numpy as jnp
from jax import lax

C = 128
SECTIONS = 4
FRAMES = 2
H = 64
W = 32
N_SEGMENT = 4


def shard_levels(key, shape, pieces, smallest, high):
    loudness, own = 1.0, jax.random.fold_in(key, 6)
    for position, shards_of in pieces:
        draws = jnp.exp(jax.random.uniform(jax.random.fold_in(own, position), (shards_of,), jnp.float32, smallest / len(pieces), high / len(pieces)))
        loudness = loudness * jnp.repeat(draws, shape[position] // shards_of).reshape([-1 if axis == position else 1 for axis in range(len(shape))])
    return loudness


def centred(own_key, extent, spread, limit, shards=(), dtype=jnp.bfloat16):
    entries = jax.random.normal(own_key, extent, jnp.float32) * spread
    if len(shards) > 0:
        entries = shard_levels(own_key, extent, shards, -0.22, 0.18) * entries
    return jnp.clip(entries, min=-limit, max=limit).astype(dtype)


def setup_inputs(seed: int = 0) -> dict:
    streams_of = jax.random.split(jax.random.key(seed), 6)
    return {
        "frames": centred(streams_of[0], (FRAMES, H, W, C), 1.0, 6.0, ((1, 4), (2, 2))),
        "caches": centred(streams_of[1], (SECTIONS, 2, 2, H, W, C), 0.7, 5.0, ((0, 4), (3, 4), (4, 2))),
        "weights": centred(streams_of[2], (SECTIONS, 2, 3, 3, 3, C, C), (27 * C) ** -0.5, 0.109375, ((0, 4),)),
        "biases": jnp.clip(jax.random.uniform(streams_of[3], (SECTIONS, 2, C), jnp.float32, -0.5, 0.5) * shard_levels(streams_of[3], (SECTIONS, 2, C), ((0, 4),), -0.4, 0.0), -0.5, 0.5),
        "gains": jnp.clip(1.0 + 0.18 * jax.random.normal(streams_of[4], (SECTIONS, 2, C), jnp.float32), 0.1, 1.9),
    }


def norm_act(values, gain_row):
    values = values.astype(jnp.float32)
    scaled = values * jax.lax.rsqrt(lax.optimization_barrier(jnp.mean(values * values, axis=-1, keepdims=True)) + 1e-06) * gain_row
    return jax.nn.silu(scaled).astype(jnp.bfloat16)

def convolve(sequence, previous, kernel, bias_row):
    joined = jnp.concatenate([previous, sequence], axis=0)
    padded = jnp.pad(joined, ((0, 0), (1, 1), (1, 1), (0, 0)))
    frame_count = sequence.shape[0]
    rows = sequence.shape[1]
    cols = sequence.shape[2]
    accum = jnp.zeros(sequence.shape[:3] + (kernel.shape[-1],), jnp.float32)
    for tap_t in range(3):
        for tap_h in range(3):
            for tap_w in range(3):
                slab = padded[tap_t:tap_t + frame_count, tap_h:tap_h + rows, tap_w:tap_w + cols].astype(jnp.float32)
                accum = accum + jnp.einsum('fhwc,co->fhwo', slab, kernel[tap_t, tap_h, tap_w].astype(jnp.float32))
    return accum + bias_row

def reference(frames, caches, weights, biases, gains):
    current = frames
    results = []
    for section in range(N_SEGMENT):
        normed_one = norm_act(current, gains[section, 0])
        hidden = convolve(normed_one, caches[section, 0], weights[section, 0], biases[section, 0])
        normed_two = norm_act(hidden, gains[section, 1])
        branch = convolve(normed_two, caches[section, 1], weights[section, 1], biases[section, 1])
        current = (current.astype(jnp.float32) + branch).astype(jnp.bfloat16)
        results.append(current)
    return jnp.stack(results, axis=0)
```

```python
import functools

import jax
import jax.numpy as jnp
from jax import lax
from jax.experimental import pallas as pl
from jax.experimental.pallas import tpu as pltpu
from jax.sharding import PartitionSpec as P

STRIP = 8
TAPS = 3
AROUND = [(dr, dc) for dr in (-1, 0, 1) for dc in (-1, 0, 1)]
CENTRE = AROUND.index((0, 0))


def divisor(count, most):
    return max(d for d in range(1, most + 1) if count % d == 0)


def source_range(step, size, width):
    return pl.ds(0, size) if step == 0 else pl.ds(0 if step < 0 else size - width, width)


def target_range(step, size, width, edge):
    if step == 0:
        return pl.ds(edge, size)
    return pl.ds(edge + size, width) if step < 0 else pl.ds(edge - width, width)


def norm_act(values, gain_row):
    scale = lax.rsqrt(jnp.mean(values * values, axis=-1, keepdims=True) + 1e-06)
    half = 0.5 * (values * scale * gain_row)
    return half * jnp.tanh(half) + half


def put_taps(store, start, values):
    size, channels = values.shape
    rows = pl.ds(start, size)
    store[rows, 0:channels] = pltpu.roll(values, 1, 0).astype(jnp.bfloat16)
    store[rows, channels : 2 * channels] = values.astype(jnp.bfloat16)
    store[rows, 2 * channels : 3 * channels] = pltpu.roll(values, size - 1, 0).astype(jnp.bfloat16)


def kernel(
    counts,
    frames, caches, weights, biases, gains,
    out,
    x_pad, one_pad, two_pad, taps_one, taps_two, sum_one, sum_two, inside,
    send_sem, recv_sem, local_sem,
):
    segments, tile_rows_n, tile_cols_n = counts
    seg, row, col = (lax.axis_index(name) for name in ("segment", "row", "col"))
    total, rows, cols, channels = frames.shape
    pitch = x_pad.shape[2]

    def exists(dr, dc):
        r, c = row + dr, col + dc
        return (r >= 0) & (r < tile_rows_n) & (c >= 0) & (c < tile_cols_n)

    def device(dz, dr, dc):
        return {"segment": seg + dz, "row": row + dr, "col": col + dc}

    def remote(source, target, halo, send_group, recv_group, dz, which):
        dr, dc = AROUND[which]
        src_r, src_c = source_range(dr, rows, halo), source_range(dc, cols, STRIP)
        dst_r, dst_c = target_range(dr, rows, halo, halo), target_range(dc, cols, STRIP, STRIP)
        lead = (slice(None),) * (len(source.shape) - 3)
        return pltpu.make_async_remote_copy(
            src_ref=source.at[lead + (src_r, src_c)],
            dst_ref=target.at[lead + (dst_r, dst_c)],
            send_sem=send_sem.at[send_group, which],
            recv_sem=recv_sem.at[recv_group, which],
            device_id=device(dz, dr, dc),
            device_id_type=pl.DeviceIdType.MESH,
        )

    streams = [
        (caches.at[0], one_pad, 2, 0, 0, 0),
        (caches.at[1], two_pad, 1, 1, 1, 0),
    ] + [(frames.at[f], x_pad.at[f], 2, 2 + f, 2 + f, 0) for f in range(total)]
    onward = [(out.at[f], x_pad.at[f], 2, 2 + total + f, 2 + f, 1) for f in range(total)]

    def each(stream, allowed, action):
        for which, (dr, dc) in enumerate(AROUND):
            if stream[5] == 0 and which == CENTRE:
                continue
            good = exists(dr, dc) if action != "recv" else exists(-dr, -dc)
            if allowed is not None:
                good = good & allowed

            @pl.when(good)
            def _():
                copy = remote(*stream, which)
                if action == "start":
                    copy.start()
                elif action == "send":
                    copy.wait_send()
                else:
                    copy.wait_recv()

    for pad, halo in ((x_pad, 2), (one_pad, 2), (two_pad, 1)):
        count = pad.shape[0]
        side = pitch - STRIP - cols
        pad[:, 0:halo] = jnp.zeros((count, halo, pitch, channels), pad.dtype)
        pad[:, halo + rows :] = jnp.zeros((count, halo, pitch, channels), pad.dtype)
        pad[:, halo : halo + rows, 0:STRIP] = jnp.zeros((count, rows, STRIP, channels), pad.dtype)
        pad[:, halo : halo + rows, STRIP + cols :] = jnp.zeros((count, rows, side, channels), pad.dtype)

    barrier = pltpu.get_barrier_semaphore()
    arrivals = 0
    for dz in (-1, 0, 1):
        for dr, dc in AROUND:
            if (dz, dr, dc) == (0, 0, 0):
                continue
            good = exists(dr, dc) & (seg + dz >= 0) & (seg + dz < segments)

            @pl.when(good)
            def _():
                pl.semaphore_signal(
                    barrier, inc=1, device_id=device(dz, dr, dc),
                    device_id_type=pl.DeviceIdType.MESH,
                )

            arrivals = arrivals + good.astype(jnp.int32)
    centre_of = lambda pad, halo: pad.at[:, pl.ds(halo, rows), pl.ds(STRIP, cols)]
    local = [
        pltpu.make_async_copy(caches.at[0], centre_of(one_pad, 2), local_sem.at[0]),
        pltpu.make_async_copy(caches.at[1], centre_of(two_pad, 1), local_sem.at[1]),
    ]
    own = pltpu.make_async_copy(frames, centre_of(x_pad, 2), local_sem.at[2])
    for copy in local:
        copy.start()
    first = seg == 0
    later = seg > 0
    more = seg < segments - 1

    @pl.when(first)
    def _():
        own.start()

    pl.semaphore_wait(barrier, arrivals)

    each(streams[0], None, "start")
    for f in range(total):
        each(streams[2 + f], first, "start")
    each(streams[1], None, "start")

    cell = lax.broadcasted_iota(jnp.int32, inside.shape, 0)
    cell_row = row * rows + cell // pitch - 1
    cell_col = col * cols + cell % pitch - STRIP
    inside[...] = jnp.where(
        (cell_row >= 0) & (cell_row < rows * tile_rows_n)
        & (cell_col >= 0) & (cell_col < cols * tile_cols_n), 1.0, 0.0,
    )

    def kernel_of(which, *times):
        return jnp.concatenate([weights[which, t] for t in times], axis=1)

    def product(store, start, size, matrix):
        patches = jnp.concatenate(
            [store[pl.ds((start + dh) * pitch, size * pitch), :] for dh in range(TAPS)], axis=1
        )
        return jnp.dot(patches, matrix, preferred_element_type=jnp.float32)

    step_in = divisor(rows + 4, 5)
    step_one = divisor(rows + 2, 6)
    step_two = divisor(rows, 4)

    def load_taps(pad, index, store, size, step, transform):
        for start in range(0, size, step):
            values = pad[index, start : start + step].reshape(step * pitch, channels)
            put_taps(store, start * pitch, transform(values.astype(jnp.float32)))

    def cached(which, pad, store, sums, size, step, tall):
        bias = biases[which : which + 1]
        load_taps(pad, 0, store, tall, divisor(tall, 5), lambda v: v)
        for start in range(0, size, step):
            part = pl.ds(start * pitch, step * pitch)
            sums[0, part] = product(store, start, step, kernel_of(which, 0)) + bias
        load_taps(pad, 1, store, tall, divisor(tall, 5), lambda v: v)
        for start in range(0, size, step):
            part = pl.ds(start * pitch, step * pitch)
            both = product(store, start, step, kernel_of(which, 1, 0))
            sums[0, part] += both[:, :channels]
            sums[1, part] = both[:, channels:] + bias

    local[0].wait()
    each(streams[0], None, "recv")
    cached(0, one_pad, taps_one, sum_one, rows + 2, step_one, rows + 4)
    local[1].wait()
    each(streams[1], None, "recv")
    cached(1, two_pad, taps_two, sum_two, rows, step_two, rows + 2)

    @pl.when(first)
    def _():
        own.wait()

    for f in range(total):
        each(streams[2 + f], first, "recv")
        each(onward[f], later, "recv")
        load_taps(x_pad, f, taps_one, rows + 4, step_in, lambda v: norm_act(v, gains[0:1]))
        times = (2, 1) if f == 0 else (2,)
        for start in range(0, rows + 2, step_one):
            part = pl.ds(start * pitch, step_one * pitch)
            fresh = product(taps_one, start, step_one, kernel_of(0, *times))
            hidden = sum_one[f, part] + fresh[:, :channels]
            if f == 0:
                sum_one[1, part] += fresh[:, channels:]
            put_taps(taps_two, start * pitch, norm_act(hidden, gains[1:2]) * inside[part])
        for start in range(0, rows, step_two):
            part = pl.ds(start * pitch, step_two * pitch)
            fresh = product(taps_two, start, step_two, kernel_of(1, *times))
            branch = sum_two[f, part] + fresh[:, :channels]
            if f == 0:
                sum_two[1, part] += fresh[:, channels:]
            branch = branch.reshape(step_two, pitch, channels)[:, STRIP : STRIP + cols]
            inputs = x_pad[f, 2 + start : 2 + start + step_two, STRIP : STRIP + cols]
            out[f, start : start + step_two] = (inputs.astype(jnp.float32) + branch).astype(out.dtype)
        each(onward[f], more, "start")

    for stream in streams[:2]:
        each(stream, None, "send")
    for f in range(total):
        each(streams[2 + f], first, "send")
        each(onward[f], more, "send")


def solution(mesh):
    counts = tuple(mesh.shape[name] for name in ("segment", "row", "col"))

    def on_device(frames, caches, weights, biases, gains):
        total, rows, cols, channels = frames.shape
        pitch = -(-(cols + 2 * STRIP) // 16) * 16
        bf16, f32 = jnp.bfloat16, jnp.float32
        vmem = pl.BlockSpec(memory_space=pltpu.VMEM)
        taps = weights.reshape(2, TAPS, TAPS * TAPS * channels, channels)
        result = pl.pallas_call(
            functools.partial(kernel, counts),
            out_shape=jax.ShapeDtypeStruct(frames.shape, bf16),
            in_specs=[vmem] * 5,
            out_specs=vmem,
            scratch_shapes=[
                pltpu.VMEM((total, rows + 4, pitch, channels), bf16),
                pltpu.VMEM((2, rows + 4, pitch, channels), bf16),
                pltpu.VMEM((2, rows + 2, pitch, channels), bf16),
                pltpu.VMEM(((rows + 4) * pitch, TAPS * channels), bf16),
                pltpu.VMEM(((rows + 2) * pitch, TAPS * channels), bf16),
                pltpu.VMEM((total, (rows + 2) * pitch, channels), f32),
                pltpu.VMEM((total, rows * pitch, channels), f32),
                pltpu.VMEM(((rows + 2) * pitch, channels), f32),
                pltpu.SemaphoreType.DMA((2 + 2 * total, 9)),
                pltpu.SemaphoreType.DMA((2 + total, 9)),
                pltpu.SemaphoreType.DMA((3,)),
            ],
            compiler_params=pltpu.CompilerParams(collective_id=0, has_side_effects=True),
        )(frames, caches[0], taps, biases[0], gains[0])
        return result[None]

    in_specs = (
        P(None, "row", "col", None),
        P("segment", None, None, "row", "col", None),
        P("segment", None, None, None, None, None, None),
        P("segment", None, None),
        P("segment", None, None),
    )
    out_specs = P("segment", None, "row", "col", None)
    return jax.shard_map(
        on_device, mesh=mesh, in_specs=in_specs, out_specs=out_specs, check_vma=False
    )
```

```python
import functools

import jax
import jax.numpy as jnp
from jax import lax
from jax.experimental import pallas as pl
from jax.experimental.pallas import tpu as pltpu
from jax.sharding import PartitionSpec as P

EDGE = 8
STRIP = 2
TAPS = 3
AROUND = [(dr, dc) for dr in (-1, 0, 1) for dc in (-1, 0, 1)]
CENTRE = AROUND.index((0, 0))


def divisor(count, most):
    return max(d for d in range(1, most + 1) if count % d == 0)


def source_range(step, size, width, edge):
    if step == 0:
        return pl.ds(edge, size)
    return pl.ds(edge if step < 0 else edge + size - width, width)


def target_range(step, size, width, edge):
    if step == 0:
        return pl.ds(edge, size)
    return pl.ds(edge + size, width) if step < 0 else pl.ds(edge - width, width)


def norm_act(values, gain_row):
    scale = lax.rsqrt(jnp.mean(values * values, axis=-1, keepdims=True) + 1e-06)
    half = 0.5 * (values * scale * gain_row)
    return half * jnp.tanh(half) + half


def put_taps(store, start, values):
    size, channels = values.shape
    rows = pl.ds(start, size)
    store[rows, 0:channels] = pltpu.roll(values, 1, 0).astype(jnp.bfloat16)
    store[rows, channels : 2 * channels] = values.astype(jnp.bfloat16)
    store[rows, 2 * channels : 3 * channels] = pltpu.roll(values, size - 1, 0).astype(jnp.bfloat16)


def kernel(
    counts,
    frames, caches, weights_in, biases_in, gains_in,
    out,
    weights, biases, gains, x_pad, one_pad, two_pad, taps_one, taps_two, sum_one, sum_two, inside,
    send_sem, recv_sem, local_sem,
):
    segments, tile_rows_n, tile_cols_n = counts
    seg, row, col = (lax.axis_index(name) for name in ("segment", "row", "col"))
    total, rows, cols, channels = frames.shape
    pitch = x_pad.shape[2]

    def exists(dr, dc):
        r, c = row + dr, col + dc
        return (r >= 0) & (r < tile_rows_n) & (c >= 0) & (c < tile_cols_n)

    def device(dz, dr, dc):
        return {"segment": seg + dz, "row": row + dr, "col": col + dc}

    def remote(source, target, halo, send_group, recv_group, dz, which):
        dr, dc = AROUND[which]
        top, left = (0, 0) if dz else (halo, EDGE)
        src_r, src_c = source_range(dr, rows, halo, top), source_range(dc, cols, STRIP, left)
        dst_r, dst_c = target_range(dr, rows, halo, halo), target_range(dc, cols, STRIP, EDGE)
        lead = (slice(None),) * (len(source.shape) - 3)
        return pltpu.make_async_remote_copy(
            src_ref=source.at[lead + (src_r, src_c)],
            dst_ref=target.at[lead + (dst_r, dst_c)],
            send_sem=send_sem.at[send_group, which],
            recv_sem=recv_sem.at[recv_group, which],
            device_id=device(dz, dr, dc),
            device_id_type=pl.DeviceIdType.MESH,
        )

    streams = [
        (one_pad, one_pad, 2, 0, 0, 0),
        (two_pad, two_pad, 1, 1, 1, 0),
    ] + [(x_pad.at[f], x_pad.at[f], 2, 2 + f, 2 + f, 0) for f in range(total)]
    onward = [(out.at[f], x_pad.at[f], 2, 2 + total + f, 2 + f, 1) for f in range(total)]

    def each(stream, allowed, action):
        for which, (dr, dc) in enumerate(AROUND):
            if stream[5] == 0 and which == CENTRE:
                continue
            good = exists(dr, dc) if action != "recv" else exists(-dr, -dc)
            if allowed is not None:
                good = good & allowed

            @pl.when(good)
            def _():
                copy = remote(*stream, which)
                if action == "start":
                    copy.start()
                elif action == "send":
                    copy.wait_send()
                else:
                    copy.wait_recv()

    centre_of = lambda pad, halo: pad.at[:, pl.ds(halo, rows), pl.ds(EDGE, cols)]
    first = seg == 0
    later = seg > 0
    more = seg < segments - 1
    own = pltpu.make_async_copy(frames, centre_of(x_pad, 2), local_sem.at[0])
    held_one = pltpu.make_async_copy(caches.at[0], centre_of(one_pad, 2), local_sem.at[1])
    held_two = pltpu.make_async_copy(caches.at[1], centre_of(two_pad, 1), local_sem.at[2])
    parameters = [
        pltpu.make_async_copy(biases_in, biases, local_sem.at[3]),
        pltpu.make_async_copy(gains_in, gains, local_sem.at[4]),
        pltpu.make_async_copy(weights_in.at[0], weights.at[0], local_sem.at[5]),
        pltpu.make_async_copy(weights_in.at[1], weights.at[1], local_sem.at[6]),
    ]

    @pl.when(first)
    def _():
        own.start()

    for copy in [held_one, held_two] + parameters:
        copy.start()

    for pad, halo in ((x_pad, 2), (one_pad, 2), (two_pad, 1)):
        count = pad.shape[0]
        side = pitch - EDGE - cols
        pad[:, 0:halo] = jnp.zeros((count, halo, pitch, channels), pad.dtype)
        pad[:, halo + rows :] = jnp.zeros((count, halo, pitch, channels), pad.dtype)
        pad[:, halo : halo + rows, 0:EDGE] = jnp.zeros((count, rows, EDGE, channels), pad.dtype)
        pad[:, halo : halo + rows, EDGE + cols :] = jnp.zeros((count, rows, side, channels), pad.dtype)

    barrier = pltpu.get_barrier_semaphore()
    arrivals = 0
    for dz in (-1, 0, 1):
        for dr, dc in AROUND:
            if (dz, dr, dc) == (0, 0, 0):
                continue
            good = exists(dr, dc) & (seg + dz >= 0) & (seg + dz < segments)

            @pl.when(good)
            def _():
                pl.semaphore_signal(
                    barrier, inc=1, device_id=device(dz, dr, dc),
                    device_id_type=pl.DeviceIdType.MESH,
                )

            arrivals = arrivals + good.astype(jnp.int32)
    pl.semaphore_wait(barrier, arrivals)

    @pl.when(first)
    def _():
        own.wait()

    for f in range(total):
        each(streams[2 + f], first, "start")
    held_one.wait()
    each(streams[0], None, "start")
    held_two.wait()
    each(streams[1], None, "start")

    cell = lax.broadcasted_iota(jnp.int32, inside.shape, 0)
    cell_row = row * rows + cell // pitch - 1
    cell_col = col * cols + cell % pitch - EDGE
    inside[...] = jnp.where(
        (cell_row >= 0) & (cell_row < rows * tile_rows_n)
        & (cell_col >= 0) & (cell_col < cols * tile_cols_n), 1.0, 0.0,
    )

    def kernel_of(which, *times):
        return jnp.concatenate([weights[which, t] for t in times], axis=1)

    def product(store, start, size, matrix):
        patches = jnp.concatenate(
            [store[pl.ds((start + dh) * pitch, size * pitch), :] for dh in range(TAPS)], axis=1
        )
        return jnp.dot(patches, matrix, preferred_element_type=jnp.float32)

    step_in = divisor(rows + 4, 5)
    step_one = divisor(rows + 2, 6)
    step_two = divisor(rows, 4)

    def load_taps(pad, index, store, size, step, transform):
        for start in range(0, size, step):
            values = pad[index, start : start + step].reshape(step * pitch, channels)
            put_taps(store, start * pitch, transform(values.astype(jnp.float32)))

    def cached(which, pad, store, sums, size, step, tall):
        bias = biases[which : which + 1]
        load_taps(pad, 0, store, tall, divisor(tall, 5), lambda v: v)
        for start in range(0, size, step):
            part = pl.ds(start * pitch, step * pitch)
            sums[0, part] = product(store, start, step, kernel_of(which, 0)) + bias
        load_taps(pad, 1, store, tall, divisor(tall, 5), lambda v: v)
        for start in range(0, size, step):
            part = pl.ds(start * pitch, step * pitch)
            both = product(store, start, step, kernel_of(which, 1, 0))
            sums[0, part] += both[:, :channels]
            sums[1, part] = both[:, channels:] + bias

    for copy in parameters:
        copy.wait()
    each(streams[0], None, "recv")
    cached(0, one_pad, taps_one, sum_one, rows + 2, step_one, rows + 4)
    each(streams[1], None, "recv")
    cached(1, two_pad, taps_two, sum_two, rows, step_two, rows + 2)

    for f in range(total):
        each(streams[2 + f], first, "recv")
        each(onward[f], later, "recv")
        load_taps(x_pad, f, taps_one, rows + 4, step_in, lambda v: norm_act(v, gains[0:1]))
        times = (2, 1) if f == 0 else (2,)
        for start in range(0, rows + 2, step_one):
            part = pl.ds(start * pitch, step_one * pitch)
            fresh = product(taps_one, start, step_one, kernel_of(0, *times))
            hidden = sum_one[f, part] + fresh[:, :channels]
            if f == 0:
                sum_one[1, part] += fresh[:, channels:]
            put_taps(taps_two, start * pitch, norm_act(hidden, gains[1:2]) * inside[part])
        for start in range(0, rows, step_two):
            part = pl.ds(start * pitch, step_two * pitch)
            fresh = product(taps_two, start, step_two, kernel_of(1, *times))
            branch = sum_two[f, part] + fresh[:, :channels]
            if f == 0:
                sum_two[1, part] += fresh[:, channels:]
            branch = branch.reshape(step_two, pitch, channels)[:, EDGE : EDGE + cols]
            inputs = x_pad[f, 2 + start : 2 + start + step_two, EDGE : EDGE + cols]
            out[f, start : start + step_two] = (inputs.astype(jnp.float32) + branch).astype(out.dtype)
        each(onward[f], more, "start")

    for stream in streams[:2]:
        each(stream, None, "send")
    for f in range(total):
        each(streams[2 + f], first, "send")
        each(onward[f], more, "send")


def solution(mesh):
    counts = tuple(mesh.shape[name] for name in ("segment", "row", "col"))

    def on_device(frames, caches, weights, biases, gains):
        total, rows, cols, channels = frames.shape
        pitch = -(-(cols + 2 * EDGE) // 16) * 16
        bf16, f32 = jnp.bfloat16, jnp.float32
        vmem = pl.BlockSpec(memory_space=pltpu.VMEM)
        taps = weights.reshape(2, TAPS, TAPS * TAPS * channels, channels)
        result = pl.pallas_call(
            functools.partial(kernel, counts),
            out_shape=pltpu.VMEM(frames.shape, bf16),
            in_specs=[pl.BlockSpec(memory_space=pl.ANY)] * 5,
            out_specs=vmem,
            scratch_shapes=[
                pltpu.VMEM(taps.shape, bf16),
                pltpu.VMEM(biases.shape[1:], f32),
                pltpu.VMEM(gains.shape[1:], f32),
                pltpu.VMEM((total, rows + 4, pitch, channels), bf16),
                pltpu.VMEM((2, rows + 4, pitch, channels), bf16),
                pltpu.VMEM((2, rows + 2, pitch, channels), bf16),
                pltpu.VMEM(((rows + 4) * pitch, TAPS * channels), bf16),
                pltpu.VMEM(((rows + 2) * pitch, TAPS * channels), bf16),
                pltpu.VMEM((total, (rows + 2) * pitch, channels), f32),
                pltpu.VMEM((total, rows * pitch, channels), f32),
                pltpu.VMEM(((rows + 2) * pitch, channels), f32),
                pltpu.SemaphoreType.DMA((2 + 2 * total, 9)),
                pltpu.SemaphoreType.DMA((2 + total, 9)),
                pltpu.SemaphoreType.DMA((7,)),
            ],
            compiler_params=pltpu.CompilerParams(collective_id=0, has_side_effects=True),
        )(frames, caches[0], taps, biases[0], gains[0])
        return result[None]

    in_specs = (
        P(None, "row", "col", None),
        P("segment", None, None, "row", "col", None),
        P("segment", None, None, None, None, None, None),
        P("segment", None, None),
        P("segment", None, None),
    )
    out_specs = P("segment", None, "row", "col", None)
    return jax.shard_map(
        on_device, mesh=mesh, in_specs=in_specs, out_specs=out_specs, check_vma=False
    )
```

```python
import functools

import jax
import jax.numpy as jnp
from jax import lax
from jax.experimental import pallas as pl
from jax.experimental.pallas import tpu as pltpu
from jax.sharding import PartitionSpec as P

EDGE = 8
STRIP = 2
TAPS = 3
AROUND = [(dr, dc) for dr in (-1, 1, 0) for dc in (-1, 1, 0)]
CENTRE = AROUND.index((0, 0))


def divisor(count, most):
    return max(d for d in range(1, most + 1) if count % d == 0)


def source_range(step, size, width, edge):
    if step == 0:
        return pl.ds(edge, size)
    return pl.ds(edge if step < 0 else edge + size - width, width)


def target_range(step, size, width, edge):
    if step == 0:
        return pl.ds(edge, size)
    return pl.ds(edge + size, width) if step < 0 else pl.ds(edge - width, width)


def norm_act(values, gain_row):
    scale = lax.rsqrt(jnp.mean(values * values, axis=-1, keepdims=True) + 1e-06)
    half = 0.5 * (values * scale * gain_row)
    return half * jnp.tanh(half) + half


def put_taps(store, start, values):
    size, channels = values.shape
    rows = pl.ds(start, size)
    store[rows, 0:channels] = pltpu.roll(values, 1, 0).astype(jnp.bfloat16)
    store[rows, channels : 2 * channels] = values.astype(jnp.bfloat16)
    store[rows, 2 * channels : 3 * channels] = pltpu.roll(values, size - 1, 0).astype(jnp.bfloat16)


def kernel(
    counts,
    frames, caches, weights_in, biases_in, gains_in,
    out,
    weights, biases, gains, x_pad, one_pad, two_pad, taps_one, taps_two,
    held_taps_one, held_taps_two, sum_one, sum_two, inside,
    send_sem, recv_sem, tile_send, tile_recv, local_sem,
):
    segments, tile_rows_n, tile_cols_n = counts
    seg, row, col = (lax.axis_index(name) for name in ("segment", "row", "col"))
    total, rows, cols, channels = frames.shape
    pitch = x_pad.shape[2]

    def exists(dr, dc):
        r, c = row + dr, col + dc
        return (r >= 0) & (r < tile_rows_n) & (c >= 0) & (c < tile_cols_n)

    def device(dz, dr, dc):
        return {"segment": seg + dz, "row": row + dr, "col": col + dc}

    def remote(source, target, halo, send_group, recv_group, dz, which):
        dr, dc = AROUND[which]
        top, left = (0, 0) if dz else (halo, EDGE)
        src_r, src_c = source_range(dr, rows, halo, top), source_range(dc, cols, STRIP, left)
        dst_r, dst_c = target_range(dr, rows, halo, halo), target_range(dc, cols, STRIP, EDGE)
        lead = (slice(None),) * (len(source.shape) - 3)
        return pltpu.make_async_remote_copy(
            src_ref=source.at[lead + (src_r, src_c)],
            dst_ref=target.at[lead + (dst_r, dst_c)],
            send_sem=send_sem.at[send_group, which],
            recv_sem=recv_sem.at[recv_group, which],
            device_id=device(dz, dr, dc),
            device_id_type=pl.DeviceIdType.MESH,
        )

    streams = [
        (one_pad, one_pad, 2, 0, 0, 0),
        (two_pad, two_pad, 1, 1, 1, 0),
    ] + [(x_pad.at[f], x_pad.at[f], 2, 2 + f, 2 + f, 0) for f in range(total)]
    onward = [(out.at[f], x_pad.at[f], 2, 2 + total + f, 2 + f, 1) for f in range(total)]

    step_in = divisor(rows + 4, 5)
    step_one = divisor(rows + 2, 6)
    step_two = divisor(rows, 4)
    chunks = rows // step_two

    def tile_copy(f, chunk):
        start = chunk * step_two
        return pltpu.make_async_remote_copy(
            src_ref=out.at[f, pl.ds(start, step_two)],
            dst_ref=x_pad.at[f, pl.ds(2 + start, step_two), pl.ds(EDGE, cols)],
            send_sem=tile_send.at[f, chunk],
            recv_sem=tile_recv.at[f, chunk],
            device_id=device(1, 0, 0),
            device_id_type=pl.DeviceIdType.MESH,
        )

    def each(stream, allowed, action, steps=(-1, 1, 0)):
        for which, (dr, dc) in enumerate(AROUND):
            if which == CENTRE or dr not in steps:
                continue
            good = exists(dr, dc) if action != "recv" else exists(-dr, -dc)
            if allowed is not None:
                good = good & allowed

            @pl.when(good)
            def _():
                copy = remote(*stream, which)
                if action == "start":
                    copy.start()
                elif action == "send":
                    copy.wait_send()
                else:
                    copy.wait_recv()

    centre_of = lambda pad, halo: pad.at[:, pl.ds(halo, rows), pl.ds(EDGE, cols)]
    first = seg == 0
    later = seg > 0
    more = seg < segments - 1
    own = pltpu.make_async_copy(frames, centre_of(x_pad, 2), local_sem.at[0])
    held_one = pltpu.make_async_copy(caches.at[0], centre_of(one_pad, 2), local_sem.at[1])
    held_two = pltpu.make_async_copy(caches.at[1], centre_of(two_pad, 1), local_sem.at[2])
    parameters = [
        pltpu.make_async_copy(biases_in, biases, local_sem.at[3]),
        pltpu.make_async_copy(gains_in, gains, local_sem.at[4]),
        pltpu.make_async_copy(weights_in.at[0], weights.at[0], local_sem.at[5]),
        pltpu.make_async_copy(weights_in.at[1], weights.at[1], local_sem.at[6]),
    ]

    @pl.when(first)
    def _():
        own.start()

    for copy in [held_one, held_two] + parameters:
        copy.start()

    for pad, halo in ((x_pad, 2), (one_pad, 2), (two_pad, 1)):
        count = pad.shape[0]
        side = pitch - EDGE - cols
        pad[:, 0:halo] = jnp.zeros((count, halo, pitch, channels), pad.dtype)
        pad[:, halo + rows :] = jnp.zeros((count, halo, pitch, channels), pad.dtype)
        pad[:, halo : halo + rows, 0:EDGE] = jnp.zeros((count, rows, EDGE, channels), pad.dtype)
        pad[:, halo : halo + rows, EDGE + cols :] = jnp.zeros((count, rows, side, channels), pad.dtype)

    barrier = pltpu.get_barrier_semaphore()
    arrivals = 0
    for dz in (-1, 0, 1):
        for dr, dc in AROUND:
            if (dz, dr, dc) == (0, 0, 0):
                continue
            good = exists(dr, dc) & (seg + dz >= 0) & (seg + dz < segments)

            @pl.when(good)
            def _():
                pl.semaphore_signal(
                    barrier, inc=1, device_id=device(dz, dr, dc),
                    device_id_type=pl.DeviceIdType.MESH,
                )

            arrivals = arrivals + good.astype(jnp.int32)
    pl.semaphore_wait(barrier, arrivals)

    @pl.when(first)
    def _():
        own.wait()

    for f in range(total):
        each(streams[2 + f], first, "start")
    held_one.wait()
    each(streams[0], None, "start")
    held_two.wait()
    each(streams[1], None, "start")

    cell = lax.broadcasted_iota(jnp.int32, inside.shape, 0)
    cell_row = row * rows + cell // pitch - 1
    cell_col = col * cols + cell % pitch - EDGE
    inside[...] = jnp.where(
        (cell_row >= 0) & (cell_row < rows * tile_rows_n)
        & (cell_col >= 0) & (cell_col < cols * tile_cols_n), 1.0, 0.0,
    )

    def kernel_of(which, *times):
        return jnp.concatenate([weights[which, t] for t in times], axis=1)

    def product(store, start, size, matrix):
        patches = jnp.concatenate(
            [store[pl.ds((start + dh) * pitch, size * pitch), :] for dh in range(TAPS)], axis=1
        )
        return jnp.dot(patches, matrix, preferred_element_type=jnp.float32)

    def load_taps(pad, index, store, size, step, transform):
        for start in range(0, size, step):
            values = pad[index, start : start + step].reshape(step * pitch, channels)
            put_taps(store, start * pitch, transform(values.astype(jnp.float32)))

    def cached(which, pad, store, sums, tap_rows, sum_rows):
        bias = biases[which : which + 1]
        for frame in range(2):
            for low, high in tap_rows:
                step = divisor(high - low, 4)
                for start in range(low, high, step):
                    values = pad[frame, start : start + step].reshape(step * pitch, channels)
                    put_taps(store.at[frame], start * pitch, values.astype(jnp.float32))
        for low, high in sum_rows:
            step = divisor(high - low, 7)
            for start in range(low, high, step):
                part = pl.ds(start * pitch, step * pitch)
                older = product(store.at[0], start, step, kernel_of(which, 0))
                newer = product(store.at[1], start, step, kernel_of(which, 1, 0))
                sums[0, part] = older + newer[:, :channels] + bias
                sums[1, part] = newer[:, channels:] + bias

    for copy in parameters:
        copy.wait()
    held = ((one_pad, held_taps_one, sum_one, 2), (two_pad, held_taps_two, sum_two, 1))
    for which, (pad, store, sums, halo) in enumerate(held):
        end = halo + rows
        each(streams[which], None, "recv", (0,))
        cached(which, pad, store, sums, [(halo, end)], [(halo, end - 2)])
    for which, (pad, store, sums, halo) in enumerate(held):
        end = halo + rows
        each(streams[which], None, "recv", (-1, 1))
        cached(
            which, pad, store, sums,
            [(0, halo), (end, end + halo)], [(0, halo), (end - 2, end + halo - 2)],
        )

    for f in range(total):
        each(streams[2 + f], first, "recv")
        each(onward[f], later, "recv")

        @pl.when(later)
        def _():
            for chunk in range(chunks):
                tile_copy(f, chunk).wait_recv()

        load_taps(x_pad, f, taps_one, rows + 4, step_in, lambda v: norm_act(v, gains[0:1]))
        times = (2, 1) if f == 0 else (2,)
        for start in range(0, rows + 2, step_one):
            part = pl.ds(start * pitch, step_one * pitch)
            fresh = product(taps_one, start, step_one, kernel_of(0, *times))
            hidden = sum_one[f, part] + fresh[:, :channels]
            if f == 0:
                sum_one[1, part] += fresh[:, channels:]
            put_taps(taps_two, start * pitch, norm_act(hidden, gains[1:2]) * inside[part])
        for chunk in [0, chunks - 1] + list(range(1, chunks - 1)) if chunks > 1 else [0]:
            start = chunk * step_two
            part = pl.ds(start * pitch, step_two * pitch)
            fresh = product(taps_two, start, step_two, kernel_of(1, *times))
            branch = sum_two[f, part] + fresh[:, :channels]
            if f == 0:
                sum_two[1, part] += fresh[:, channels:]
            branch = branch.reshape(step_two, pitch, channels)[:, EDGE : EDGE + cols]
            inputs = x_pad[f, 2 + start : 2 + start + step_two, EDGE : EDGE + cols]
            out[f, start : start + step_two] = (inputs.astype(jnp.float32) + branch).astype(out.dtype)
            if chunk == 0:
                each(onward[f], more, "start", (-1,))
            if chunk == chunks - 1:
                each(onward[f], more, "start", (1,))

            @pl.when(more)
            def _():
                tile_copy(f, chunk).start()

        each(onward[f], more, "start", (0,))

    for stream in streams[:2]:
        each(stream, None, "send")
    for f in range(total):
        each(streams[2 + f], first, "send")
        each(onward[f], more, "send")

        @pl.when(more)
        def _():
            for chunk in range(chunks):
                tile_copy(f, chunk).wait_send()


def solution(mesh):
    counts = tuple(mesh.shape[name] for name in ("segment", "row", "col"))

    def on_device(frames, caches, weights, biases, gains):
        total, rows, cols, channels = frames.shape
        pitch = -(-(cols + 2 * EDGE) // 16) * 16
        bf16, f32 = jnp.bfloat16, jnp.float32
        vmem = pl.BlockSpec(memory_space=pltpu.VMEM)
        taps = weights.reshape(2, TAPS, TAPS * TAPS * channels, channels)
        result = pl.pallas_call(
            functools.partial(kernel, counts),
            out_shape=pltpu.VMEM(frames.shape, bf16),
            in_specs=[pl.BlockSpec(memory_space=pl.ANY)] * 5,
            out_specs=vmem,
            scratch_shapes=[
                pltpu.VMEM(taps.shape, bf16),
                pltpu.VMEM(biases.shape[1:], f32),
                pltpu.VMEM(gains.shape[1:], f32),
                pltpu.VMEM((total, rows + 4, pitch, channels), bf16),
                pltpu.VMEM((2, rows + 4, pitch, channels), bf16),
                pltpu.VMEM((2, rows + 2, pitch, channels), bf16),
                pltpu.VMEM(((rows + 4) * pitch, TAPS * channels), bf16),
                pltpu.VMEM(((rows + 2) * pitch, TAPS * channels), bf16),
                pltpu.VMEM((2, (rows + 4) * pitch, TAPS * channels), bf16),
                pltpu.VMEM((2, (rows + 2) * pitch, TAPS * channels), bf16),
                pltpu.VMEM((total, (rows + 2) * pitch, channels), f32),
                pltpu.VMEM((total, rows * pitch, channels), f32),
                pltpu.VMEM(((rows + 2) * pitch, channels), f32),
                pltpu.SemaphoreType.DMA((2 + 2 * total, 9)),
                pltpu.SemaphoreType.DMA((2 + total, 9)),
                pltpu.SemaphoreType.DMA((total, divisor(rows, 16))),
                pltpu.SemaphoreType.DMA((total, divisor(rows, 16))),
                pltpu.SemaphoreType.DMA((7,)),
            ],
            compiler_params=pltpu.CompilerParams(collective_id=0, has_side_effects=True),
        )(frames, caches[0], taps, biases[0], gains[0])
        return result[None]

    in_specs = (
        P(None, "row", "col", None),
        P("segment", None, None, "row", "col", None),
        P("segment", None, None, None, None, None, None),
        P("segment", None, None),
        P("segment", None, None),
    )
    out_specs = P("segment", None, "row", "col", None)
    return jax.shard_map(
        on_device, mesh=mesh, in_specs=in_specs, out_specs=out_specs, check_vma=False
    )
```
